32 devices in a mesh: tok: 8 (over z, x), mp: 4 (over y, core).
Axes of the slice: x: 2, y: 2, z: 4, core: 2. Of those that a mesh axis runs over, the one named last changes fastest.
Arguments:
- tokens: bfloat16 [3072, 2048], P('tok', 'mp'), may hold values from -120 to 120
- norm_gain: float32 [2048], replicated, may hold values from 0.5 to 1.5
- running_sq: float32 [2048], P('mp'), may hold values from 0.5 to 4
- gate_weight: bfloat16 [2048, 8192], P(None, 'mp'), may hold values from -0.125 to 0.125
- up_weight: bfloat16 [2048, 8192], P(None, 'mp'), may hold values from -0.125 to 0.125
- down_weight_t: bfloat16 [2048, 8192], P(None, 'mp'), may hold values from -0.0625 to 0.0625
- groups: int32 [192], P('tok'), may hold values from 0 to 23, as said below
- cotangent: bfloat16 [3072, 2048], P('tok', 'mp'), may hold values from -6 to 6
Outputs:
- block_out: bfloat16 [3072, 2048], P('tok', 'mp')
- grad_tokens: bfloat16 [3072, 2048], P('tok', 'mp')
- running_new: float32 [2048], P('mp')
- grad_gain: float32 [2048], P('mp')
- grad_gate: float32 [2048, 8192], P('tok', 'mp')
- grad_up: float32 [2048, 8192], P('tok', 'mp')
- grad_down_t: float32 [2048, 8192], P('tok', 'mp')
The draws below stay inside these ranges and needn't reach their ends.
Inputs may be any that keep to these rules, and one draw needn't show every extreme that they name: Each of the 24 ghost groups holds exactly 8 blocks.
All inputs are finite; a program needn't handle non-finite values.
Results may differ from the reference program's by a relative error of at most 0.02.
Values may be sent and summed in bfloat16 or wider, within the bound.
A program may use at most 128 MiB of HBM per device.

```python
import math
import jax
import jax.numpy as jnp
from jax import lax

D = 2048
FF = 8192
GHOST = 128
BLK = 16
TOKENS = 3072
GROUPS = 24
NBLK = 192


def draw_groups(key, part):
    blocks_per_group = GHOST // BLK
    order = jax.random.permutation(jax.random.fold_in(key, 11), NBLK)
    return (order // blocks_per_group).astype(jnp.int32)


def draw_tokens(key, part):
    key_base, key_block, key_column = jax.random.split(jax.random.fold_in(key, 23), 3)
    position = jnp.arange(TOKENS, dtype=jnp.float32)
    rising = jnp.exp(jnp.log(3.0) * position / TOKENS)
    block_scale = jnp.exp(jax.random.uniform(key_block, (NBLK,), jnp.float32, jnp.log(0.5), jnp.log(2.0)))
    row_scale = jnp.broadcast_to(block_scale[:, None], (NBLK, BLK)).reshape(TOKENS) * rising
    column_scale = jnp.exp(jax.random.uniform(key_column, (D,), jnp.float32, jnp.log(0.3), jnp.log(3.0)))
    base = jnp.clip(jax.random.normal(key_base, (TOKENS, D), jnp.float32), -6.0, 6.0)
    return (base * row_scale[:, None] * column_scale[None, :]).astype(jnp.bfloat16)


def level_of(stream_key, dims, pieces, low, top_value):
    def one(dim, shards_of):
        draws = jax.random.uniform(jax.random.fold_in(jax.random.fold_in(stream_key, 6), dim), (shards_of,), jnp.float32, low / len(pieces), top_value / len(pieces))
        return jnp.repeat(jnp.exp(draws), dims[dim] // shards_of).reshape((-1,) + (1,) * (len(dims) - dim - 1))

    loudness = one(*pieces[0])
    for cut in pieces[1:]:
        loudness = loudness * one(*cut)
    return loudness


def noise(rng, extent, width, bound, shards=(), kind=jnp.bfloat16):
    array = jax.random.normal(rng, extent, jnp.float32) * width
    if len(shards) > 0:
        array = level_of(rng, extent, shards, -0.22, 0.18) * array
    return jnp.clip(array, min=-bound, max=bound).astype(kind)


def setup_inputs(seed: int = 0) -> dict:
    key_of = jax.random.split(jax.random.key(seed), 9)
    return {
        "tokens": draw_tokens(jax.random.fold_in(key_of[8], 71), 0),
        "norm_gain": jnp.clip(1.0 + 0.1 * jax.random.normal(key_of[1], (D,), jnp.float32), 0.5, 1.5),
        "running_sq": jnp.clip(jnp.exp(math.log(4.0) - 2.0794415 * jax.random.uniform(key_of[2], (D,), jnp.float32) ** level_of(key_of[2], (D,), ((0, 4),), -0.2, 0.2)), 0.5, 4.0),
        "gate_weight": noise(key_of[3], (D, FF), D ** -0.5, 0.125, ((1, 4),)),
        "up_weight": noise(key_of[4], (D, FF), D ** -0.5, 0.125, ((1, 4),)),
        "down_weight_t": noise(key_of[5], (D, FF), FF ** -0.5, 0.0625, ((1, 4),)),
        "groups": draw_groups(jax.random.fold_in(key_of[8], 71), 0),
        "cotangent": noise(key_of[7], (TOKENS, D), 1.0, 6.0, ((0, 8), (1, 4))),
    }


epsilon = 1e-05
momentum = 0.1
highest = lax.Precision.HIGHEST

def group_onehot(groups):
    return (groups[None, :] == jnp.arange(GROUPS, dtype=jnp.int32)[:, None]).astype(jnp.float32)

def group_sums(values, onehot):
    blocks = values.reshape(values.shape[0] // BLK, BLK, values.shape[1]).sum(axis=1)
    return jnp.dot(onehot, blocks, precision=highest, preferred_element_type=jnp.float32)

def per_token(table, onehot):
    per_block = jnp.dot(onehot.T, table, precision=highest, preferred_element_type=jnp.float32)
    wide = jnp.broadcast_to(per_block[:, None, :], (per_block.shape[0], BLK, per_block.shape[1]))
    return wide.reshape(per_block.shape[0] * BLK, per_block.shape[1])

def reference(tokens, norm_gain, running_sq, gate_weight, up_weight, down_weight_t, groups, cotangent):
    onehot = group_onehot(groups)
    x_float = tokens.astype(jnp.float32)
    quad_mean = group_sums(x_float * x_float, onehot) / GHOST
    scale = per_token(lax.rsqrt(quad_mean + epsilon), onehot)
    normed = x_float * scale
    hid_in = (norm_gain * normed).astype(jnp.bfloat16)
    gate = jnp.dot(hid_in, gate_weight, preferred_element_type=jnp.float32)
    lift = jnp.dot(hid_in, up_weight, preferred_element_type=jnp.float32)
    sigma = jax.nn.sigmoid(gate)
    hidden = (gate * sigma * lift).astype(jnp.bfloat16)
    branch = lax.dot_general(hidden, down_weight_t, (((1,), (1,)), ((), ())), preferred_element_type=jnp.float32)
    block_out = (x_float + branch).astype(jnp.bfloat16)
    running_new = (1.0 - momentum) * running_sq + momentum * lax.optimization_barrier(jnp.mean(quad_mean, axis=0))
    grad_down_t = lax.dot_general(cotangent, hidden, (((0,), (0,)), ((), ())), preferred_element_type=jnp.float32)
    grad_hidden = jnp.dot(cotangent, down_weight_t, preferred_element_type=jnp.float32)
    grad_gate_in = (grad_hidden * lift * sigma * (1.0 + gate * (1.0 - sigma))).astype(jnp.bfloat16)
    grad_lift = (grad_hidden * gate * sigma).astype(jnp.bfloat16)
    grad_gate = lax.dot_general(hid_in, grad_gate_in, (((0,), (0,)), ((), ())), preferred_element_type=jnp.float32)
    grad_up = lax.dot_general(hid_in, grad_lift, (((0,), (0,)), ((), ())), preferred_element_type=jnp.float32)
    grad_normed_in = lax.dot_general(grad_gate_in, gate_weight, (((1,), (1,)), ((), ())), preferred_element_type=jnp.float32)
    grad_normed_in = grad_normed_in + lax.dot_general(grad_lift, up_weight, (((1,), (1,)), ((), ())), preferred_element_type=jnp.float32)
    partial_value = group_sums(grad_normed_in * normed, onehot)
    grad_gain = lax.optimization_barrier(jnp.sum(partial_value, axis=0))
    mean_term = per_token(norm_gain * partial_value / GHOST, onehot)
    grad_tokens = (cotangent.astype(jnp.float32) + scale * (norm_gain * grad_normed_in - normed * mean_term)).astype(jnp.bfloat16)
    return (block_out, grad_tokens, running_new, grad_gain, grad_gate, grad_up, grad_down_t)
```

```python
import functools

import jax
import jax.numpy as jnp
from jax import lax
from jax.experimental import pallas as pl
from jax.experimental.pallas import tpu as pltpu
from jax.sharding import PartitionSpec as P

GHOST = 128
BLK = 16
EPSILON = 1e-05
MOMENTUM = 0.1
Z = 4
CORES = 2
MESH = pl.DeviceIdType.MESH
F32 = jnp.float32
BF16 = jnp.bfloat16


def dot(a, b, ca=1, cb=0, precision=None):
    return lax.dot_general(
        a, b, (((ca,), (cb,)), ((), ())), precision=precision, preferred_element_type=F32
    )


def kernel(
    tok_count,
    mp_count,
    x_ref,
    gain_ref,
    run_ref,
    groups_ref,
    dy_ref,
    wg_hbm,
    wu_hbm,
    wd_hbm,
    bo_ref,
    gt_ref,
    rn_ref,
    gg_ref,
    dgate_hbm,
    dup_hbm,
    ddown_hbm,
    wa,
    wb,
    hg,
    dg,
    hidden,
    ggi,
    gl,
    ht,
    dt,
    rbuf,
    mp_recv,
    stage,
    sblk,
    stat_x,
    stat_z,
    part_x,
    part_z,
    own_b,
    own_g,
    w_sem,
    zs,
    zr,
    ys,
    yr,
    cs,
    cr,
    sx_s,
    sx_r,
    sz_s,
    sz_r,
    px_s,
    px_r,
    pz_s,
    pz_r,
    rs_s,
    rs_r,
    ms_s,
    ms_r,
    o_sem,
):
    rows_t, feat = x_ref.shape
    width = wa.shape[1]
    full = feat * mp_count
    xs = tok_count // Z
    rows = full // tok_count
    ys_count = mp_count // CORES
    nb = rows_t // BLK
    groups_total = rows_t * tok_count // GHOST

    me = lax.axis_index("tok")
    m = lax.axis_index("mp")
    z, x = me // xs, me % xs
    y, c = m // CORES, m % CORES

    def z_peer(k):
        zz = z + 0
        if k & 1:
            zz = zz + 1 - 2 * (zz % 2)
        if k & 2:
            zz = (zz + 2) % Z
        return (zz * xs + x, m)

    def x_peer(j):
        return (z * xs + (x + j) % xs, m)

    def y_peer(j):
        return (me, ((y + j) % ys_count) * CORES + c)

    core_peer = (me, y * CORES + (1 - c))

    def mp_peer(j):
        return (me, (m + j) % mp_count)

    def remote(src, dst, s, r, dev):
        return pltpu.make_async_remote_copy(
            src_ref=src, dst_ref=dst, send_sem=s, recv_sem=r, device_id=dev, device_id_type=MESH
        )

    load_a = pltpu.make_async_copy(wg_hbm, wa, w_sem.at[0])
    load_b = pltpu.make_async_copy(wu_hbm, wb, w_sem.at[1])
    load_a.start()
    load_b.start()

    barrier = pltpu.get_barrier_semaphore()
    greet = [z_peer(k) for k in range(1, Z)] + [x_peer(j) for j in range(1, xs)]
    greet += [mp_peer(j) for j in range(1, mp_count)]
    for dev in greet:
        pl.semaphore_signal(barrier, inc=1, device_id=dev, device_id_type=MESH)
    pl.semaphore_wait(barrier, len(greet))

    bufs = (hg, dg)

    def block(a, k, owner):
        col = pl.multiple_of(owner * feat, feat)
        return bufs[a].at[pl.ds(k * rows_t, rows_t), pl.ds(col, feat)]

    def z_copy(a, k):
        return remote(block(a, 0, m), block(a, k, m), zs.at[a, k], zr.at[a, k], z_peer(k))

    def y_copy(a, k, j):
        return remote(block(a, k, m), block(a, k, m), ys.at[a, k, j], yr.at[a, k, j], y_peer(j))

    def y_from(j):
        return ((y + ys_count - j) % ys_count) * CORES + c

    def y_wait(a, k, j):
        b = block(a, k, y_from(j))
        remote(b, b, ys.at[a, k, j], yr.at[a, k, j], y_peer(j)).wait_recv()

    def c_copy(a, k, i):
        b = block(a, k, y_from(i))
        return remote(b, b, cs.at[a, k, i], cr.at[a, k, i], core_peer)

    def c_wait(a, k, i):
        b = block(a, k, ((y + ys_count - i) % ys_count) * CORES + (1 - c))
        remote(b, b, cs.at[a, k, i], cr.at[a, k, i], core_peer).wait_recv()

    def forward_y(a, k):
        if k > 0:
            b = block(a, k, m)
            remote(b, b, zs.at[a, k], zr.at[a, k], z_peer(k)).wait_recv()
        for j in range(1, ys_count):
            y_copy(a, k, j).start()
        c_copy(a, k, 0).start()

    def forward_c(a, k):
        for j in range(1, ys_count):
            y_wait(a, k, j)
            c_copy(a, k, j).start()

    def ready(a, k):
        for i in range(ys_count):
            c_wait(a, k, i)

    def sent(a):
        for k in range(Z):
            if k > 0:
                z_copy(a, k).wait_send()
            for j in range(1, ys_count):
                y_copy(a, k, j).wait_send()
            for i in range(ys_count):
                c_copy(a, k, i).wait_send()

    own_cols = pl.ds(pl.multiple_of(m * feat, feat), feat)
    dg[pl.ds(0, rows_t), own_cols] = dy_ref[...]
    forward_y(1, 0)

    groups = groups_ref[...]
    onehot = (lax.broadcasted_iota(jnp.int32, (groups_total, nb), 0) == groups).astype(F32)

    def group_sums(values):
        blocks = values.reshape(nb, BLK, feat).sum(axis=1)
        return dot(onehot, blocks, precision=lax.Precision.HIGHEST)

    def per_block(table):
        return dot(onehot, table, 0, 0, precision=lax.Precision.HIGHEST)

    def per_token(blocks):
        wide = jnp.broadcast_to(blocks[:, None, :], (nb, BLK, feat))
        return wide.reshape(rows_t, feat)

    def exchange_start(buf, slot, s, r, count, peer):
        for j in range(1, count):
            remote(buf.at[slot], buf.at[slot], s.at[j], r.at[j], peer(j)).start()

    def exchange_sum(buf, slot, s, r, count, peer):
        for j in range(1, count):
            remote(buf.at[slot], buf.at[slot], s.at[j], r.at[j], peer(j)).wait()
        total = buf[0]
        for j in range(1, count):
            total = total + buf[j]
        return total

    def tok_total(value, bx, bz, xsend, xrecv, zsend, zrecv):
        bx[x] = value
        exchange_start(bx, x, xsend, xrecv, xs, x_peer)
        bz[z] = exchange_sum(bx, x, xsend, xrecv, xs, x_peer)
        exchange_start(bz, z, zsend, zrecv, Z, z_peer)
        return exchange_sum(bz, z, zsend, zrecv, Z, z_peer)

    xf = x_ref[...].astype(F32)
    quad_mean = tok_total(group_sums(xf * xf), stat_x, stat_z, sx_s, sx_r, sz_s, sz_r) / GHOST
    gain = gain_ref[m]
    sblk[...] = per_block(lax.rsqrt(quad_mean + EPSILON))
    normed = x_ref[...].astype(F32) * per_token(sblk[...])
    hg[pl.ds(0, rows_t), own_cols] = (gain * normed).astype(BF16)
    mean_q = jnp.sum(quad_mean, axis=0, keepdims=True) / groups_total
    rn_ref[...] = (1.0 - MOMENTUM) * run_ref[...] + MOMENTUM * mean_q

    forward_y(0, 0)
    for k in range(1, Z):
        z_copy(0, k).start()
    for k in range(1, Z):
        z_copy(1, k).start()
    forward_c(1, 0)
    ready(1, 0)

    tile = min(256, width)
    steps = width // tile

    def cols(n, size):
        return pl.ds(pl.multiple_of(n * size, size), size)

    load_a.wait()
    load_b.wait()
    for k in range(Z):
        forward_c(0, k)
        if k + 1 < Z:
            forward_y(0, k + 1)
        else:
            forward_y(1, 1)
        ready(0, k)
        part = pl.ds(k * rows_t, rows_t)

        def hidden_tile(n, carry):
            w = cols(n, tile)
            gate = dot(hg[part, :], wa[:, w])
            lift = dot(hg[part, :], wb[:, w])
            sigma = 1.0 / (1.0 + jnp.exp(-gate))
            act = gate * sigma
            hidden[part, w] = (act * lift).astype(BF16)
            ggi[part, w] = (lift * sigma * (1.0 + gate * (1.0 - sigma))).astype(BF16)
            gl[part, w] = act.astype(BF16)
            return carry

        lax.fori_loop(0, steps, hidden_tile, 0)

    load_d = pltpu.make_async_copy(wd_hbm, wa, w_sem.at[0])
    load_d.start()

    def transposed(src, dst):
        for j in range(xs):
            first = (z * xs + (x + j) % xs) * rows
            lanes = pl.ds(pl.multiple_of(first, rows), rows)
            for k in range(Z):
                part = pl.ds(k * rows_t, rows_t)
                value = src[part, lanes].astype(F32).T.astype(BF16)
                dst[pl.ds(j * rows, rows), part] = value

    transposed(hg, ht)
    load_d.wait()

    for k in range(Z):
        if k > 0:
            forward_c(1, k)
        if 0 < k < Z - 1:
            forward_y(1, k + 1)
        if k > 0:
            ready(1, k)
        part = pl.ds(k * rows_t, rows_t)

        def gradient_tile(n, carry):
            w = cols(n, tile)
            gh = dot(dg[part, :], wa[:, w])
            ggi[part, w] = (gh * ggi[part, w].astype(F32)).astype(BF16)
            gl[part, w] = (gh * gl[part, w].astype(F32)).astype(BF16)
            return carry

        lax.fori_loop(0, steps, gradient_tile, 0)

    transposed(dg, dt)
    sent(0)
    sent(1)

    big = min(512, width)
    sides = ((ht, ggi), (ht, gl), (dt, hidden))
    other = (xs - 1) * rows

    def rs_copy(w, j):
        src = hg.at[pl.ds((w * (xs - 1) + j - 1) * rows, rows), pl.ds(0, width)]
        return remote(src, rbuf.at[w, j - 1], rs_s.at[w, j], rs_r.at[w, j], x_peer(j))

    def rs_compute(w):
        left, right = sides[w]

        def rs_tile(n, carry):
            lanes = cols(n, big)
            value = dot(left[pl.ds(rows, other), :], right[:, lanes])
            hg[pl.ds(w * other, other), lanes] = value.astype(BF16)
            return carry

        lax.fori_loop(0, width // big, rs_tile, 0)

    def rs_start(w):
        for j in range(1, xs):
            rs_copy(w, j).start()

    rs_compute(0)
    rs_start(0)
    rs_compute(1)
    rs_start(1)

    def m_copy(a, j):
        src = dg.at[pl.ds(a * rows_t, rows_t), pl.ds((j - 1) * feat, feat)]
        return remote(src, mp_recv.at[a, j - 1], ms_s.at[a, j], ms_r.at[a, j], mp_peer(j))

    def over_hidden(a, terms, own):
        def one(j, start):
            first = pl.multiple_of(((m + j) % mp_count) * feat, feat)
            value = None
            for left, weight in terms:
                more = dot(left[pl.ds(0, rows_t), :], weight[pl.ds(first, feat), :], 1, 1)
                value = more if value is None else value + more
            return value

        for j in range(1, mp_count):
            dg[pl.ds(a * rows_t, rows_t), pl.ds((j - 1) * feat, feat)] = one(j, 0).astype(BF16)
            m_copy(a, j).start()
        own[...] = one(0, 0)

    def received(a, own):
        total = own[...]
        for j in range(1, mp_count):
            m_copy(a, j).wait()
            total = total + mp_recv[a, j - 1].astype(F32)
        return total

    over_hidden(0, ((hidden, wa),), own_b)
    load_g = pltpu.make_async_copy(wg_hbm, wa, w_sem.at[0])
    load_g.start()
    rs_compute(2)
    load_g.wait()
    over_hidden(1, ((ggi, wa), (gl, wb)), own_g)
    bo_ref[...] = (x_ref[...].astype(F32) + received(0, own_b)).astype(BF16)
    own_g[...] = received(1, own_g)
    normed = x_ref[...].astype(F32) * per_token(sblk[...])
    part_x[x] = group_sums(own_g[...] * normed)
    exchange_start(part_x, x, px_s, px_r, xs, x_peer)
    rs_start(2)
    part_z[z] = exchange_sum(part_x, x, px_s, px_r, xs, x_peer)
    exchange_start(part_z, z, pz_s, pz_r, Z, z_peer)
    total = exchange_sum(part_z, z, pz_s, pz_r, Z, z_peer)
    gg_ref[...] = jnp.sum(total, axis=0, keepdims=True)
    scale = per_token(sblk[...])
    normed = x_ref[...].astype(F32) * scale
    mean_term = per_token(per_block(gain * total / GHOST))
    gt_ref[...] = (
        dy_ref[...].astype(F32) + scale * (gain * own_g[...] - normed * mean_term)
    ).astype(BF16)

    outs = (dgate_hbm, dup_hbm, ddown_hbm)
    pending = {}
    count = 0
    for w in range(3):
        for j in range(1, xs):
            rs_copy(w, j).wait()
        left, right = sides[w]
        for n in range(width // big):
            slot = count % 2
            if slot in pending:
                pending[slot].wait()
            lanes = pl.ds(n * big, big)
            value = dot(left[pl.ds(0, rows), :], right[:, lanes])
            for j in range(1, xs):
                value = value + rbuf[w, j - 1, :, lanes].astype(F32)
            stage[slot] = value
            copy = pltpu.make_async_copy(stage.at[slot], outs[w].at[:, lanes], o_sem.at[slot])
            copy.start()
            pending[slot] = copy
            count += 1
    for copy in pending.values():
        copy.wait()


def body(tokens, norm_gain, running_sq, gate_weight, up_weight, down_weight_t, groups, cotangent):
    tok_count, mp_count = lax.axis_size("tok"), lax.axis_size("mp")
    rows_t, feat = tokens.shape
    full, width = gate_weight.shape
    xs = tok_count // Z
    rows = full // tok_count
    nb = rows_t // BLK
    groups_total = rows_t * tok_count // GHOST
    ys_count = mp_count // CORES
    big = min(512, width)
    vmem = pl.BlockSpec(memory_space=pltpu.VMEM)
    hbm = pl.BlockSpec(memory_space=pl.ANY)
    dma = pltpu.SemaphoreType.DMA
    table = (groups_total, feat)
    grad = jax.ShapeDtypeStruct((rows, width), F32)
    outs = pl.pallas_call(
        functools.partial(kernel, tok_count, mp_count),
        out_shape=(
            jax.ShapeDtypeStruct((rows_t, feat), BF16),
            jax.ShapeDtypeStruct((rows_t, feat), BF16),
            jax.ShapeDtypeStruct((1, feat), F32),
            jax.ShapeDtypeStruct((1, feat), F32),
            grad,
            grad,
            grad,
        ),
        in_specs=[vmem] * 5 + [hbm] * 3,
        out_specs=(vmem,) * 4 + (hbm,) * 3,
        scratch_shapes=[
            pltpu.VMEM((full, width), BF16),
            pltpu.VMEM((full, width), BF16),
            pltpu.VMEM((Z * rows_t, full), BF16),
            pltpu.VMEM((Z * rows_t, full), BF16),
            pltpu.VMEM((Z * rows_t, width), BF16),
            pltpu.VMEM((Z * rows_t, width), BF16),
            pltpu.VMEM((Z * rows_t, width), BF16),
            pltpu.VMEM((xs * rows, Z * rows_t), BF16),
            pltpu.VMEM((xs * rows, Z * rows_t), BF16),
            pltpu.VMEM((3, xs - 1, rows, width), BF16),
            pltpu.VMEM((2, mp_count - 1, rows_t, feat), BF16),
            pltpu.VMEM((2, rows, big), F32),
            pltpu.VMEM((nb, feat), F32),
            pltpu.VMEM((xs,) + table, F32),
            pltpu.VMEM((Z,) + table, F32),
            pltpu.VMEM((xs,) + table, F32),
            pltpu.VMEM((Z,) + table, F32),
            pltpu.VMEM((rows_t, feat), F32),
            pltpu.VMEM((rows_t, feat), F32),
            dma((2,)),
            dma((2, Z)),
            dma((2, Z)),
            dma((2, Z, ys_count)),
            dma((2, Z, ys_count)),
            dma((2, Z, ys_count)),
            dma((2, Z, ys_count)),
            dma((xs,)),
            dma((xs,)),
            dma((Z,)),
            dma((Z,)),
            dma((xs,)),
            dma((xs,)),
            dma((Z,)),
            dma((Z,)),
            dma((3, xs)),
            dma((3, xs)),
            dma((2, mp_count)),
            dma((2, mp_count)),
            dma((2,)),
        ],
        compiler_params=pltpu.CompilerParams(
            collective_id=0, has_side_effects=True, vmem_limit_bytes=67043328
        ),
        name="sublayer",
    )(
        tokens,
        norm_gain.reshape(mp_count, 1, feat),
        running_sq.reshape(1, feat),
        groups.reshape(1, nb),
        cotangent,
        gate_weight,
        up_weight,
        down_weight_t,
    )
    block_out, grad_tokens, running_new, grad_gain, grad_gate, grad_up, grad_down_t = outs
    return (
        block_out,
        grad_tokens,
        running_new.reshape(feat),
        grad_gain.reshape(feat),
        grad_gate,
        grad_up,
        grad_down_t,
    )


def solution(mesh):
    placed = (
        P("tok", "mp"),
        P(),
        P("mp"),
        P(None, "mp"),
        P(None, "mp"),
        P(None, "mp"),
        P("tok"),
        P("tok", "mp"),
    )
    return jax.shard_map(
        body,
        mesh=mesh,
        in_specs=placed,
        out_specs=(
            P("tok", "mp"),
            P("tok", "mp"),
            P("mp"),
            P("mp"),
            P("tok", "mp"),
            P("tok", "mp"),
            P("tok", "mp"),
        ),
        check_vma=False,
    )
```

```python
import functools

import jax
import jax.numpy as jnp
from jax import lax
from jax.experimental import pallas as pl
from jax.experimental.pallas import tpu as pltpu
from jax.sharding import PartitionSpec as P

GHOST = 128
BLK = 16
EPSILON = 1e-05
MOMENTUM = 0.1
Z = 4
CORES = 2
MESH = pl.DeviceIdType.MESH
F32 = jnp.float32
BF16 = jnp.bfloat16


def dot(a, b, ca=1, cb=0, precision=None):
    return lax.dot_general(
        a, b, (((ca,), (cb,)), ((), ())), precision=precision, preferred_element_type=F32
    )


def kernel(
    tok_count,
    mp_count,
    x_ref,
    gain_ref,
    run_ref,
    groups_ref,
    dy_ref,
    wg_hbm,
    wu_hbm,
    wd_hbm,
    bo_ref,
    gt_ref,
    rn_ref,
    gg_ref,
    own_hbm,
    recv_hbm,
    wa,
    wb,
    hg,
    dg,
    hidden,
    ggi,
    gl,
    ht,
    dt,
    mp_recv,
    stage,
    sblk,
    stat_x,
    stat_z,
    part_x,
    part_z,
    own_b,
    own_g,
    w_sem,
    zs,
    zr,
    ys,
    yr,
    cs,
    cr,
    sx_s,
    sx_r,
    sz_s,
    sz_r,
    px_s,
    px_r,
    pz_s,
    pz_r,
    rs_s,
    rs_r,
    ms_s,
    ms_r,
    o_sem,
):
    rows_t, feat = x_ref.shape
    width = wa.shape[1]
    full = feat * mp_count
    xs = tok_count // Z
    rows = full // tok_count
    ys_count = mp_count // CORES
    nb = rows_t // BLK
    groups_total = rows_t * tok_count // GHOST

    me = lax.axis_index("tok")
    m = lax.axis_index("mp")
    z, x = me // xs, me % xs
    y, c = m // CORES, m % CORES

    inner = (z == 1) | (z == 2)

    def z_peer(k):
        zz = z + 0
        if k & 1:
            zz = zz + 1 - 2 * (zz % 2)
        if k & 2:
            zz = (zz + 2) % Z
        return (zz * xs + x, m)

    def x_peer(j):
        return (z * xs + (x + j) % xs, m)

    def y_peer(j):
        return (me, ((y + j) % ys_count) * CORES + c)

    core_peer = (me, y * CORES + (1 - c))

    def mp_peer(j):
        return (me, (m + j) % mp_count)

    def remote(src, dst, s, r, dev):
        return pltpu.make_async_remote_copy(
            src_ref=src, dst_ref=dst, send_sem=s, recv_sem=r, device_id=dev, device_id_type=MESH
        )

    load_a = pltpu.make_async_copy(wg_hbm, wa, w_sem.at[0])
    load_b = pltpu.make_async_copy(wu_hbm, wb, w_sem.at[1])
    load_a.start()
    load_b.start()

    barrier = pltpu.get_barrier_semaphore()
    greet = [z_peer(k) for k in range(1, Z)] + [x_peer(j) for j in range(1, xs)]
    greet += [mp_peer(j) for j in range(1, mp_count)]
    for dev in greet:
        pl.semaphore_signal(barrier, inc=1, device_id=dev, device_id_type=MESH)
    pl.semaphore_wait(barrier, len(greet))

    bufs = (hg, dg)

    def block(a, k, owner):
        col = pl.multiple_of(owner * feat, feat)
        return bufs[a].at[pl.ds(k * rows_t, rows_t), pl.ds(col, feat)]

    to_near, to_mid, near_to_mid, mid_to_near, far_to_near = (
        (0, 0, 1, 1), (1, 0, 3, 3), (2, 1, 2, 3), (3, 3, 2, 1), (4, 2, 3, 1)
    )

    def z_copy(a, hop):
        slot, held, there, k = hop
        return remote(
            block(a, held, m), block(a, there, m), zs.at[a, slot], zr.at[a, there], z_peer(k)
        )

    def z_wait(a, k):
        b = block(a, k, m)
        remote(b, b, zs.at[a, 0], zr.at[a, k], z_peer(1)).wait_recv()

    def z_own(a):
        z_copy(a, to_near).start()

        @pl.when(inner)
        def _():
            z_copy(a, to_mid).start()

    def z_first(a):
        z_wait(a, 1)

        @pl.when(inner)
        def _():
            z_copy(a, near_to_mid).start()

        forward_y(a, 1)

        @pl.when(inner)
        def _():
            z_wait(a, 3)
            z_copy(a, mid_to_near).start()
            forward_y(a, 3)

    def z_second(a):
        z_wait(a, 2)

        @pl.when(inner)
        def _():
            z_copy(a, far_to_near).start()

        forward_y(a, 2)

    outer = jnp.logical_not(inner)

    def z_third(a):
        @pl.when(outer)
        def _():
            z_wait(a, 3)
            forward_y(a, 3)

    def y_copy(a, k, j):
        return remote(block(a, k, m), block(a, k, m), ys.at[a, k, j], yr.at[a, k, j], y_peer(j))

    def y_from(j):
        return ((y + ys_count - j) % ys_count) * CORES + c

    def y_wait(a, k, j):
        b = block(a, k, y_from(j))
        remote(b, b, ys.at[a, k, j], yr.at[a, k, j], y_peer(j)).wait_recv()

    def c_copy(a, k, i):
        b = block(a, k, y_from(i))
        return remote(b, b, cs.at[a, k, i], cr.at[a, k, i], core_peer)

    def c_wait(a, k, i):
        b = block(a, k, ((y + ys_count - i) % ys_count) * CORES + (1 - c))
        remote(b, b, cs.at[a, k, i], cr.at[a, k, i], core_peer).wait_recv()

    def forward_y(a, k):
        for j in range(1, ys_count):
            y_copy(a, k, j).start()
        c_copy(a, k, 0).start()

    def wanted(owner, at=z):
        return (owner * feat) // (xs * rows) == at

    def holds(at):
        return (at * xs * rows) // (feat * CORES) == y

    near = z + 1 - 2 * (z % 2)
    first_out = wanted(m)
    alone = jnp.logical_not(holds(z))
    early = first_out | alone
    late = jnp.logical_not(early)
    near_late = holds(near) & jnp.logical_not(wanted(m, near))
    near_early = jnp.logical_not(near_late)

    def take(k):
        z_wait(1, k)
        forward_y(1, k)

    def forward_c(a, k, choose=None):
        for j in range(1, ys_count):

            def go(j=j):
                y_wait(a, k, j)
                c_copy(a, k, j).start()

            if choose is None:
                go()
            else:
                pl.when(wanted(y_from(j)) == choose)(go)

    def ready(a, k, choose=None):
        for i in range(ys_count):
            owner = ((y + ys_count - i) % ys_count) * CORES + (1 - c)
            if choose is None:
                c_wait(a, k, i)
            else:
                pl.when(wanted(owner) == choose)(functools.partial(c_wait, a, k, i))

    def chunk_sent(a, k):
        for j in range(1, ys_count):
            y_copy(a, k, j).wait_send()
        for i in range(ys_count):
            c_copy(a, k, i).wait_send()

    def own_sent(a):
        z_copy(a, to_near).wait_send()

        @pl.when(inner)
        def _():
            z_copy(a, to_mid).wait_send()

        chunk_sent(a, 0)

    def rest_sent(a):
        @pl.when(inner)
        def _():
            for which in (near_to_mid, mid_to_near, far_to_near):
                z_copy(a, which).wait_send()

        for k in range(1, Z):
            chunk_sent(a, k)

    own_cols = pl.ds(pl.multiple_of(m * feat, feat), feat)
    dg[pl.ds(0, rows_t), own_cols] = dy_ref[...]
    forward_y(1, 0)

    groups = groups_ref[...]
    onehot = (lax.broadcasted_iota(jnp.int32, (groups_total, nb), 0) == groups).astype(F32)

    def group_sums(values):
        blocks = values.reshape(nb, BLK, feat).sum(axis=1)
        return dot(onehot, blocks, precision=lax.Precision.HIGHEST)

    def per_block(table):
        return dot(onehot, table, 0, 0, precision=lax.Precision.HIGHEST)

    def per_token(blocks):
        wide = jnp.broadcast_to(blocks[:, None, :], (nb, BLK, feat))
        return wide.reshape(rows_t, feat)

    def exchange_start(buf, slot, s, r, count, peer):
        for j in range(1, count):
            remote(buf.at[slot], buf.at[slot], s.at[j], r.at[j], peer(j)).start()

    def exchange_sum(buf, slot, s, r, count, peer):
        for j in range(1, count):
            remote(buf.at[slot], buf.at[slot], s.at[j], r.at[j], peer(j)).wait()
        total = buf[0]
        for j in range(1, count):
            total = total + buf[j]
        return total

    def tok_total(value, bx, bz, xsend, xrecv, zsend, zrecv):
        bx[x] = value
        exchange_start(bx, x, xsend, xrecv, xs, x_peer)
        bz[z] = exchange_sum(bx, x, xsend, xrecv, xs, x_peer)
        exchange_start(bz, z, zsend, zrecv, Z, z_peer)
        return exchange_sum(bz, z, zsend, zrecv, Z, z_peer)

    xf = x_ref[...].astype(F32)
    quad_mean = tok_total(group_sums(xf * xf), stat_x, stat_z, sx_s, sx_r, sz_s, sz_r) / GHOST
    gain = gain_ref[m]
    sblk[...] = per_block(lax.rsqrt(quad_mean + EPSILON))
    normed = x_ref[...].astype(F32) * per_token(sblk[...])
    hg[pl.ds(0, rows_t), own_cols] = (gain * normed).astype(BF16)
    mean_q = jnp.sum(quad_mean, axis=0, keepdims=True) / groups_total
    rn_ref[...] = (1.0 - MOMENTUM) * run_ref[...] + MOMENTUM * mean_q

    z_own(0)
    forward_y(0, 0)
    forward_c(1, 0)
    ready(1, 0)

    tile = min(512, width // 2)
    steps = width // tile

    def cols(n, size):
        return pl.ds(pl.multiple_of(n * size, size), size)

    def hidden_half(k, first, last):
        part = pl.ds(k * rows_t, rows_t)

        def hidden_tile(n, carry):
            w = cols(n, tile)
            gate = dot(hg[part, :], wa[:, w])
            lift = dot(hg[part, :], wb[:, w])
            sigma = 1.0 / (1.0 + jnp.exp(-gate))
            act = gate * sigma
            hidden[part, w] = (act * lift).astype(BF16)
            ggi[part, w] = (lift * sigma * (1.0 + gate * (1.0 - sigma))).astype(BF16)
            gl[part, w] = act.astype(BF16)
            return carry

        lax.fori_loop(first, last, hidden_tile, 0)

    def at_once(flag, *calls):
        @pl.when(flag)
        def _():
            for call, arg in calls:
                call(arg)

    def hop(which):
        z_copy(1, which).start()

    def hold(k):
        z_wait(1, k)

    def pass_on(k):
        forward_y(1, k)

    load_a.wait()
    load_b.wait()
    forward_c(0, 0)
    z_first(0)
    at_once(outer, (hop, to_near))
    at_once(inner, (hop, to_mid))
    ready(0, 0)
    hidden_half(0, 0, steps)
    z_second(0)
    at_once(inner & near_early, (hop, to_near))
    forward_c(0, 1)
    ready(0, 1)
    hidden_half(1, 0, steps)
    z_third(0)
    at_once(inner, (hold, 1), (hop, near_to_mid), (hold, 3))
    at_once(inner & near_early, (hop, mid_to_near))
    at_once(inner & near_late, (hop, to_near))
    at_once(inner & early, (pass_on, 1), (pass_on, 3))
    forward_c(0, 2)
    ready(0, 2)
    hidden_half(2, 0, steps // 2)
    at_once(inner, (hold, 2))
    at_once(inner & near_early, (hop, far_to_near))
    at_once(inner & near_late, (hop, mid_to_near))
    at_once(inner & early, (pass_on, 2))
    at_once(outer & early, (take, 1))
    hidden_half(2, steps // 2, steps)
    at_once(inner & near_late, (hop, far_to_near))
    forward_c(0, 3)
    at_once(outer & early, (take, 2))
    at_once(inner & late, (pass_on, 1), (pass_on, 3))
    ready(0, 3)
    at_once(outer & late, (take, 1))
    hidden_half(3, 0, steps // 2)
    at_once(outer & early, (take, 3))
    at_once(inner & late, (pass_on, 2))
    at_once(outer & late, (take, 2))
    hidden_half(3, steps // 2, steps)
    at_once(outer & late, (take, 3))

    load_d = pltpu.make_async_copy(wd_hbm, wa, w_sem.at[0])
    load_d.start()

    def transposed(src, dst):
        for j in range(xs):
            first = (z * xs + (x + j) % xs) * rows
            lanes = pl.ds(pl.multiple_of(first, rows), rows)
            for k in range(Z):
                part = pl.ds(k * rows_t, rows_t)
                value = src[part, lanes].astype(F32).T.astype(BF16)
                dst[pl.ds(j * rows, rows), part] = value

    transposed(hg, ht)
    for k in range(1, Z):
        forward_c(1, k, True)
    for k in range(1, Z):
        ready(1, k, True)
    transposed(dg, dt)
    own_sent(0)
    rest_sent(0)

    big = min(512, width // 2)
    sides = ((ht, ggi), (ht, gl), (dt, hidden))
    other = (xs - 1) * rows
    halves = 2
    half = width // halves

    def rs_copy(w, j, h):
        lanes = pl.ds(h * half, half)
        src = hg.at[pl.ds((w * (xs - 1) + j - 1) * rows, rows), lanes]
        dst = recv_hbm.at[w, j - 1, :, lanes]
        return remote(src, dst, rs_s.at[w, j, h], rs_r.at[w, j, h], x_peer(j))

    def rs_compute(w, h):
        left, right = sides[w]
        each = half // big

        def rs_tile(n, carry):
            lanes = cols(n, big)
            value = dot(left[pl.ds(rows, other), :], right[:, lanes])
            hg[pl.ds(w * other, other), lanes] = value.astype(BF16)
            return carry

        lax.fori_loop(h * each, (h + 1) * each, rs_tile, 0)

    def rs_start(w, h):
        for j in range(1, xs):
            rs_copy(w, j, h).start()

    def m_copy(a, j):
        src = dg.at[pl.ds(a * rows_t, rows_t), pl.ds((j - 1) * feat, feat)]
        return remote(src, mp_recv.at[a, j - 1], ms_s.at[a, j], ms_r.at[a, j], mp_peer(j))

    def over_hidden(a, terms, own, send):
        def one(j):
            first = pl.multiple_of(((m + j) % mp_count) * feat, feat)
            value = None
            for left, weight in terms:
                more = dot(left[pl.ds(0, rows_t), :], weight[pl.ds(first, feat), :], 1, 1)
                value = more if value is None else value + more
            return value

        for j in range(1, mp_count):
            dg[pl.ds(a * rows_t, rows_t), pl.ds((j - 1) * feat, feat)] = one(j).astype(BF16)
            if send:
                m_copy(a, j).start()
        own[...] = one(0)

    def received(a, own):
        total = own[...]
        for j in range(1, mp_count):
            m_copy(a, j).wait()
            total = total + mp_recv[a, j - 1].astype(F32)
        return total

    pending = {}
    turn = [0]

    def own_rows(w):
        left, right = sides[w]
        for n in range(width // big):
            slot = turn[0] % 2
            if slot in pending:
                pending[slot].wait()
            lanes = pl.ds(n * big, big)
            stage[slot] = dot(left[pl.ds(0, rows), :], right[:, lanes])
            copy = pltpu.make_async_copy(stage.at[slot], own_hbm.at[w, :, lanes], o_sem.at[slot])
            copy.start()
            pending[slot] = copy
            turn[0] += 1

    for h in range(halves):
        rs_compute(2, h)
        rs_start(2, h)
    load_d.wait()

    def gradient_part(k, first, last):
        part = pl.ds(k * rows_t, rows_t)

        def gradient_tile(n, carry):
            w = cols(n, tile)
            gh = dot(dg[part, :], wa[:, w])
            ggi[part, w] = (gh * ggi[part, w].astype(F32)).astype(BF16)
            gl[part, w] = (gh * gl[part, w].astype(F32)).astype(BF16)
            return carry

        lax.fori_loop(first, last, gradient_tile, 0)

    forward_c(1, 1, False)
    gradient_part(0, 0, steps)
    forward_c(1, 2, False)
    own_sent(1)
    over_hidden(0, ((hidden, wa),), own_b, False)
    ready(1, 1, False)
    gradient_part(1, 0, steps)
    forward_c(1, 3, False)
    ready(1, 2, False)
    gradient_part(2, 0, steps)
    ready(1, 3, False)
    gradient_part(Z - 1, 0, steps // 2)
    rs_compute(0, 0)
    rs_start(0, 0)
    gradient_part(Z - 1, steps // 2, steps)
    load_g = pltpu.make_async_copy(wg_hbm, wa, w_sem.at[0])
    load_g.start()
    rs_compute(1, 0)
    rs_start(1, 0)
    rs_compute(0, 1)
    rs_start(0, 1)
    rs_compute(1, 1)
    rest_sent(1)
    load_g.wait()
    over_hidden(1, ((ggi, wa), (gl, wb)), own_g, True)
    for j in range(1, mp_count):
        m_copy(0, j).start()
    for w in range(3):
        own_rows(w)
    for copy in pending.values():
        copy.wait()
    own_g[...] = received(1, own_g)
    normed = x_ref[...].astype(F32) * per_token(sblk[...])
    part_x[x] = group_sums(own_g[...] * normed)
    exchange_start(part_x, x, px_s, px_r, xs, x_peer)
    rs_start(1, 1)
    part_z[z] = exchange_sum(part_x, x, px_s, px_r, xs, x_peer)
    exchange_start(part_z, z, pz_s, pz_r, Z, z_peer)
    total = exchange_sum(part_z, z, pz_s, pz_r, Z, z_peer)
    gg_ref[...] = jnp.sum(total, axis=0, keepdims=True)
    scale = per_token(sblk[...])
    normed = x_ref[...].astype(F32) * scale
    mean_term = per_token(per_block(gain * total / GHOST))
    gt_ref[...] = (
        dy_ref[...].astype(F32) + scale * (gain * own_g[...] - normed * mean_term)
    ).astype(BF16)
    bo_ref[...] = (x_ref[...].astype(F32) + received(0, own_b)).astype(BF16)
    for w in range(3):
        for j in range(1, xs):
            for h in range(halves):
                rs_copy(w, j, h).wait()


def finish(own, recv, bo, gt, rn, gg, bo_out, gt_out, rn_out, gg_out, dgate, dup, ddown):
    for w, out in enumerate((dgate, dup, ddown)):
        value = own[w]
        for j in range(recv.shape[1]):
            value = value + recv[w, j].astype(F32)
        out[...] = value

    @pl.when(pl.program_id(0) == 0)
    def _():
        bo_out[...] = bo[...]
        gt_out[...] = gt[...]
        rn_out[...] = rn[...]
        gg_out[...] = gg[...]


def body(tokens, norm_gain, running_sq, gate_weight, up_weight, down_weight_t, groups, cotangent):
    tok_count, mp_count = lax.axis_size("tok"), lax.axis_size("mp")
    rows_t, feat = tokens.shape
    full, width = gate_weight.shape
    xs = tok_count // Z
    rows = full // tok_count
    nb = rows_t // BLK
    groups_total = rows_t * tok_count // GHOST
    ys_count = mp_count // CORES
    big = min(512, width // 2)
    vmem = pl.BlockSpec(memory_space=pltpu.VMEM)
    hbm = pl.BlockSpec(memory_space=pl.ANY)
    dma = pltpu.SemaphoreType.DMA
    table = (groups_total, feat)
    small = (
        jax.ShapeDtypeStruct((rows_t, feat), BF16),
        jax.ShapeDtypeStruct((rows_t, feat), BF16),
        jax.ShapeDtypeStruct((1, feat), F32),
        jax.ShapeDtypeStruct((1, feat), F32),
    )
    outs = pl.pallas_call(
        functools.partial(kernel, tok_count, mp_count),
        out_shape=small
        + (
            jax.ShapeDtypeStruct((3, rows, width), F32),
            jax.ShapeDtypeStruct((3, xs - 1, rows, width), BF16),
        ),
        in_specs=[vmem] * 5 + [hbm] * 3,
        out_specs=(vmem,) * 4 + (hbm,) * 2,
        scratch_shapes=[
            pltpu.VMEM((full, width), BF16),
            pltpu.VMEM((full, width), BF16),
            pltpu.VMEM((Z * rows_t, full), BF16),
            pltpu.VMEM((Z * rows_t, full), BF16),
            pltpu.VMEM((Z * rows_t, width), BF16),
            pltpu.VMEM((Z * rows_t, width), BF16),
            pltpu.VMEM((Z * rows_t, width), BF16),
            pltpu.VMEM((xs * rows, Z * rows_t), BF16),
            pltpu.VMEM((xs * rows, Z * rows_t), BF16),
            pltpu.VMEM((2, mp_count - 1, rows_t, feat), BF16),
            pltpu.VMEM((2, rows, big), F32),
            pltpu.VMEM((nb, feat), F32),
            pltpu.VMEM((xs,) + table, F32),
            pltpu.VMEM((Z,) + table, F32),
            pltpu.VMEM((xs,) + table, F32),
            pltpu.VMEM((Z,) + table, F32),
            pltpu.VMEM((rows_t, feat), F32),
            pltpu.VMEM((rows_t, feat), F32),
            dma((2,)),
            dma((2, 5)),
            dma((2, Z)),
            dma((2, Z, ys_count)),
            dma((2, Z, ys_count)),
            dma((2, Z, ys_count)),
            dma((2, Z, ys_count)),
            dma((xs,)),
            dma((xs,)),
            dma((Z,)),
            dma((Z,)),
            dma((xs,)),
            dma((xs,)),
            dma((Z,)),
            dma((Z,)),
            dma((3, xs, 2)),
            dma((3, xs, 2)),
            dma((2, mp_count)),
            dma((2, mp_count)),
            dma((2,)),
        ],
        compiler_params=pltpu.CompilerParams(
            collective_id=0, has_side_effects=True, vmem_limit_bytes=67043328
        ),
        name="sublayer",
    )(
        tokens,
        norm_gain.reshape(mp_count, 1, feat),
        running_sq.reshape(1, feat),
        groups.reshape(1, nb),
        cotangent,
        gate_weight,
        up_weight,
        down_weight_t,
    )
    block_out, grad_tokens, running_new, grad_gain, own, recv = outs
    span = min(512, width)
    whole = [pl.BlockSpec(leaf.shape, lambda n: (0, 0)) for leaf in small]
    grad = jax.ShapeDtypeStruct((rows, width), F32)
    block_out, grad_tokens, running_new, grad_gain, grad_gate, grad_up, grad_down_t = pl.pallas_call(
        finish,
        grid=(width // span,),
        out_shape=small + (grad,) * 3,
        in_specs=[
            pl.BlockSpec((3, rows, span), lambda n: (0, 0, n)),
            pl.BlockSpec((3, xs - 1, rows, span), lambda n: (0, 0, 0, n)),
        ]
        + whole,
        out_specs=whole + [pl.BlockSpec((rows, span), lambda n: (0, n))] * 3,
        name="finish",
    )(own, recv, block_out, grad_tokens, running_new, grad_gain)
    return (
        block_out,
        grad_tokens,
        running_new.reshape(feat),
        grad_gain.reshape(feat),
        grad_gate,
        grad_up,
        grad_down_t,
    )


def solution(mesh):
    placed = (
        P("tok", "mp"),
        P(),
        P("mp"),
        P(None, "mp"),
        P(None, "mp"),
        P(None, "mp"),
        P("tok"),
        P("tok", "mp"),
    )
    return jax.shard_map(
        body,
        mesh=mesh,
        in_specs=placed,
        out_specs=(
            P("tok", "mp"),
            P("tok", "mp"),
            P("mp"),
            P("mp"),
            P("tok", "mp"),
            P("tok", "mp"),
            P("tok", "mp"),
        ),
        check_vma=False,
    )
```

```python
import functools

import jax
import jax.numpy as jnp
from jax import lax
from jax.experimental import pallas as pl
from jax.experimental.pallas import tpu as pltpu
from jax.sharding import PartitionSpec as P

GHOST = 128
BLK = 16
EPSILON = 1e-05
MOMENTUM = 0.1
Z = 4
CORES = 2
MESH = pl.DeviceIdType.MESH
F32 = jnp.float32
BF16 = jnp.bfloat16


def dot(a, b, ca=1, cb=0, precision=None):
    return lax.dot_general(
        a, b, (((ca,), (cb,)), ((), ())), precision=precision, preferred_element_type=F32
    )


def kernel(
    tok_count,
    mp_count,
    x_ref,
    gain_ref,
    run_ref,
    groups_ref,
    dy_ref,
    wg_hbm,
    wu_hbm,
    wd_hbm,
    bo_ref,
    gt_ref,
    rn_ref,
    gg_ref,
    own_hbm,
    recv_hbm,
    wa,
    wb,
    hg,
    dg,
    hidden,
    ggi,
    gl,
    ht,
    dt,
    mp_recv,
    stage,
    sblk,
    stat_x,
    stat_z,
    part_x,
    part_z,
    own_b,
    own_g,
    w_sem,
    zs,
    zr,
    ys,
    yr,
    cs,
    cr,
    sx_s,
    sx_r,
    sz_s,
    sz_r,
    px_s,
    px_r,
    pz_s,
    pz_r,
    rs_s,
    rs_r,
    ms_s,
    ms_r,
    o_sem,
):
    rows_t, feat = x_ref.shape
    width = wa.shape[1]
    full = feat * mp_count
    xs = tok_count // Z
    rows = full // tok_count
    ys_count = mp_count // CORES
    nb = rows_t // BLK
    groups_total = rows_t * tok_count // GHOST

    me = lax.axis_index("tok")
    m = lax.axis_index("mp")
    z, x = me // xs, me % xs
    y, c = m // CORES, m % CORES

    inner = (z == 1) | (z == 2)

    def z_peer(k):
        zz = z + 0
        if k & 1:
            zz = zz + 1 - 2 * (zz % 2)
        if k & 2:
            zz = (zz + 2) % Z
        return (zz * xs + x, m)

    def x_peer(j):
        return (z * xs + (x + j) % xs, m)

    def y_peer(j):
        return (me, ((y + j) % ys_count) * CORES + c)

    core_peer = (me, y * CORES + (1 - c))

    def mp_peer(j):
        return (me, (m + j) % mp_count)

    def remote(src, dst, s, r, dev):
        return pltpu.make_async_remote_copy(
            src_ref=src, dst_ref=dst, send_sem=s, recv_sem=r, device_id=dev, device_id_type=MESH
        )

    load_a = pltpu.make_async_copy(wg_hbm, wa, w_sem.at[0])
    load_b = pltpu.make_async_copy(wu_hbm, wb, w_sem.at[1])
    load_a.start()
    load_b.start()

    barrier = pltpu.get_barrier_semaphore()
    greet = [z_peer(k) for k in range(1, Z)] + [x_peer(j) for j in range(1, xs)]
    greet += [mp_peer(j) for j in range(1, mp_count)]
    for dev in greet:
        pl.semaphore_signal(barrier, inc=1, device_id=dev, device_id_type=MESH)
    pl.semaphore_wait(barrier, len(greet))

    bufs = (hg, dg)

    def block(a, k, owner):
        col = pl.multiple_of(owner * feat, feat)
        return bufs[a].at[pl.ds(k * rows_t, rows_t), pl.ds(col, feat)]

    to_near, to_mid, near_to_mid, mid_to_near, far_to_near = (
        (0, 0, 1, 1), (1, 0, 3, 3), (2, 1, 2, 3), (3, 3, 2, 1), (4, 2, 3, 1)
    )

    def z_copy(a, hop):
        slot, held, there, k = hop
        return remote(
            block(a, held, m), block(a, there, m), zs.at[a, slot], zr.at[a, there], z_peer(k)
        )

    piece = rows_t // 2

    def early_copy(i):
        col = pl.ds(pl.multiple_of(m * feat, feat), feat)
        src = dg.at[pl.ds(i * piece, piece), col]
        dst = dg.at[pl.ds(rows_t + i * piece, piece), col]
        return remote(src, dst, zs.at[1, 5 * i], zr.at[1, 1 + (Z - 1) * i], z_peer(1))

    def early_wait(i):
        col = pl.ds(pl.multiple_of(m * feat, feat), feat)
        b = dg.at[pl.ds(rows_t + i * piece, piece), col]
        remote(b, b, zs.at[1, 5 * i], zr.at[1, 1 + (Z - 1) * i], z_peer(1)).wait_recv()

    def z_wait(a, k):
        if a == 1 and k == 1:
            early_wait(0)
            early_wait(1)
            return
        b = block(a, k, m)
        remote(b, b, zs.at[a, 0], zr.at[a, k], z_peer(1)).wait_recv()

    def z_own(a):
        z_copy(a, to_near).start()

        @pl.when(inner)
        def _():
            z_copy(a, to_mid).start()

    def z_first(a):
        z_wait(a, 1)

        @pl.when(inner)
        def _():
            z_copy(a, near_to_mid).start()

        forward_y(a, 1)

        @pl.when(inner)
        def _():
            z_wait(a, 3)
            z_copy(a, mid_to_near).start()

    def z_second(a):
        z_wait(a, 2)

        @pl.when(inner)
        def _():
            z_copy(a, far_to_near).start()

        forward_y(a, 2)

    outer = jnp.logical_not(inner)

    def z_third(a):
        @pl.when(outer)
        def _():
            z_wait(a, 3)

        forward_y(a, 3)

    def y_copy(a, k, j):
        return remote(block(a, k, m), block(a, k, m), ys.at[a, k, j], yr.at[a, k, j], y_peer(j))

    def y_from(j):
        return ((y + ys_count - j) % ys_count) * CORES + c

    def y_wait(a, k, j):
        b = block(a, k, y_from(j))
        remote(b, b, ys.at[a, k, j], yr.at[a, k, j], y_peer(j)).wait_recv()

    def c_copy(a, k, i):
        b = block(a, k, y_from(i))
        return remote(b, b, cs.at[a, k, i], cr.at[a, k, i], core_peer)

    def c_wait(a, k, i):
        b = block(a, k, ((y + ys_count - i) % ys_count) * CORES + (1 - c))
        remote(b, b, cs.at[a, k, i], cr.at[a, k, i], core_peer).wait_recv()

    def forward_y(a, k):
        for j in range(1, ys_count):
            y_copy(a, k, j).start()
        c_copy(a, k, 0).start()

    def wanted(owner, at=z):
        return (owner * feat) // (xs * rows) == at

    def holds(at):
        return (at * xs * rows) // (feat * CORES) == y

    first_out = wanted(m)
    alone = jnp.logical_not(holds(z))
    early = first_out | alone
    late = jnp.logical_not(early)
    near = z + 1 - 2 * (z % 2)
    near_late = holds(near) & jnp.logical_not(wanted(m, near))
    near_early = jnp.logical_not(near_late)

    def take(k):
        z_wait(1, k)
        forward_y(1, k)

    def forward_c(a, k, choose=None):
        for j in range(1, ys_count):

            def go(j=j):
                y_wait(a, k, j)
                c_copy(a, k, j).start()

            if choose is None:
                go()
            else:
                pl.when(wanted(y_from(j)) == choose)(go)

    def ready(a, k, choose=None):
        for i in range(ys_count):
            owner = ((y + ys_count - i) % ys_count) * CORES + (1 - c)
            if choose is None:
                c_wait(a, k, i)
            else:
                pl.when(wanted(owner) == choose)(functools.partial(c_wait, a, k, i))

    def chunk_sent(a, k):
        for j in range(1, ys_count):
            y_copy(a, k, j).wait_send()
        for i in range(ys_count):
            c_copy(a, k, i).wait_send()

    def own_sent(a):
        if a == 1:
            early_copy(0).wait_send()
            early_copy(1).wait_send()
        else:
            z_copy(a, to_near).wait_send()

        @pl.when(inner)
        def _():
            z_copy(a, to_mid).wait_send()

        chunk_sent(a, 0)

    def rest_sent(a):
        @pl.when(inner)
        def _():
            for which in (near_to_mid, mid_to_near, far_to_near):
                z_copy(a, which).wait_send()

        for k in range(1, Z):
            chunk_sent(a, k)

    own_cols = pl.ds(pl.multiple_of(m * feat, feat), feat)
    dg[pl.ds(0, rows_t), own_cols] = dy_ref[...]
    early_copy(0).start()
    forward_y(1, 0)

    groups = groups_ref[...]
    onehot = (lax.broadcasted_iota(jnp.int32, (groups_total, nb), 0) == groups).astype(F32)

    def group_sums(values):
        blocks = values.reshape(nb, BLK, feat).sum(axis=1)
        return dot(onehot, blocks, precision=lax.Precision.HIGHEST)

    def per_block(table):
        return dot(onehot, table, 0, 0, precision=lax.Precision.HIGHEST)

    def per_token(blocks):
        wide = jnp.broadcast_to(blocks[:, None, :], (nb, BLK, feat))
        return wide.reshape(rows_t, feat)

    def exchange_start(buf, slot, s, r, count, peer):
        for j in range(1, count):
            remote(buf.at[slot], buf.at[slot], s.at[j], r.at[j], peer(j)).start()

    def exchange_sum(buf, slot, s, r, count, peer):
        for j in range(1, count):
            remote(buf.at[slot], buf.at[slot], s.at[j], r.at[j], peer(j)).wait()
        total = buf[0]
        for j in range(1, count):
            total = total + buf[j]
        return total

    xf = x_ref[...].astype(F32)
    stat_x[x] = group_sums(xf * xf)
    exchange_start(stat_x, x, sx_s, sx_r, xs, x_peer)
    stat_z[z] = exchange_sum(stat_x, x, sx_s, sx_r, xs, x_peer)
    exchange_start(stat_z, z, sz_s, sz_r, Z, z_peer)
    early_copy(1).start()
    quad_mean = exchange_sum(stat_z, z, sz_s, sz_r, Z, z_peer) / GHOST
    gain = gain_ref[m]
    sblk[...] = per_block(lax.rsqrt(quad_mean + EPSILON))
    normed = x_ref[...].astype(F32) * per_token(sblk[...])
    hg[pl.ds(0, rows_t), own_cols] = (gain * normed).astype(BF16)
    mean_q = jnp.sum(quad_mean, axis=0, keepdims=True) / groups_total
    rn_ref[...] = (1.0 - MOMENTUM) * run_ref[...] + MOMENTUM * mean_q

    z_own(0)
    forward_y(0, 0)
    forward_c(1, 0)
    ready(1, 0)

    tile = min(512, width // 2)
    steps = width // tile

    def cols(n, size):
        return pl.ds(pl.multiple_of(n * size, size), size)

    def hidden_half(k, first, last):
        part = pl.ds(k * rows_t, rows_t)

        def hidden_tile(n, carry):
            w = cols(n, tile)
            gate = dot(hg[part, :], wa[:, w])
            lift = dot(hg[part, :], wb[:, w])
            sigma = 1.0 / (1.0 + jnp.exp(-gate))
            act = gate * sigma
            hidden[part, w] = (act * lift).astype(BF16)
            ggi[part, w] = (lift * sigma * (1.0 + gate * (1.0 - sigma))).astype(BF16)
            gl[part, w] = act.astype(BF16)
            return carry

        lax.fori_loop(first, last, hidden_tile, 0)

    def at_once(flag, *calls):
        @pl.when(flag)
        def _():
            for call, arg in calls:
                call(arg)

    def hop(which):
        z_copy(1, which).start()

    def hold(k):
        z_wait(1, k)

    def pass_on(k):
        forward_y(1, k)

    def transposed(src, dst):
        for j in range(xs):
            first = (z * xs + (x + j) % xs) * rows
            lanes = pl.ds(pl.multiple_of(first, rows), rows)
            for k in range(Z):
                part = pl.ds(k * rows_t, rows_t)
                value = src[part, lanes].astype(F32).T.astype(BF16)
                dst[pl.ds(j * rows, rows), part] = value

    at_once(first_out, (take, 1))
    load_a.wait()
    load_b.wait()
    forward_c(0, 0)
    z_first(0)
    at_once(inner & first_out, (hop, to_mid), (hop, near_to_mid))
    at_once(inner & jnp.logical_not(first_out), (hop, to_mid), (hold, 1), (hop, near_to_mid))
    ready(0, 0)
    hidden_half(0, 0, steps)
    z_second(0)
    forward_c(0, 1)
    ready(0, 1)
    hidden_half(1, 0, steps)
    z_third(0)
    at_once(inner, (hold, 3))
    at_once(inner & near_early, (hop, mid_to_near))
    at_once(inner & first_out, (pass_on, 3))
    at_once(inner & alone, (pass_on, 1), (pass_on, 3))
    at_once(outer & jnp.logical_not(first_out), (take, 1))
    forward_c(0, 2)
    ready(0, 2)
    hidden_half(2, 0, steps // 2)
    at_once(inner, (hold, 2))
    at_once(inner & near_early, (hop, far_to_near))
    at_once(inner & near_late, (hop, mid_to_near))
    at_once(inner & early, (pass_on, 2))
    hidden_half(2, steps // 2, steps)
    at_once(inner & near_late, (hop, far_to_near))
    forward_c(0, 3)
    at_once(outer & early, (take, 2))
    ready(0, 3)
    hidden_half(3, 0, steps // 2)
    at_once(outer & first_out, (take, 3))
    at_once(inner & late, (pass_on, 1), (pass_on, 3))

    big = min(512, width // 2)
    sides = ((ht, ggi), (ht, gl), (dt, hidden))
    other = (xs - 1) * rows
    halves = 2
    half = width // halves

    def rs_copy(w, j, h):
        lanes = pl.ds(h * half, half)
        src = hg.at[pl.ds((w * (xs - 1) + j - 1) * rows, rows), lanes]
        dst = recv_hbm.at[w, j - 1, :, lanes]
        return remote(src, dst, rs_s.at[w, j, h], rs_r.at[w, j, h], x_peer(j))

    def rs_compute(w, h):
        left, right = sides[w]
        each = half // big

        def rs_tile(n, carry):
            lanes = cols(n, big)
            value = dot(left[pl.ds(rows, other), :], right[:, lanes])
            hg[pl.ds(w * other, other), lanes] = value.astype(BF16)
            return carry

        lax.fori_loop(h * each, (h + 1) * each, rs_tile, 0)

    def rs_start(w, h):
        for j in range(1, xs):
            rs_copy(w, j, h).start()

    def m_copy(a, j, dev):
        src = dg.at[pl.ds(a * rows_t, rows_t), pl.ds((j - 1) * feat, feat)]
        return remote(src, mp_recv.at[a, j - 1], ms_s.at[a, j], ms_r.at[a, j], dev)

    def to_core(a, i):
        return m_copy(a, 1 + i, core_peer)

    def to_row(a, i):
        return m_copy(a, ys_count + i, y_peer(i))

    def row_share(a, i, value):
        to_core(a, i).wait_recv()
        value = value + mp_recv[a, i].astype(F32)
        first = (ys_count + i - 1) * feat
        dg[pl.ds(a * rows_t, rows_t), pl.ds(first, feat)] = value.astype(BF16)
        to_row(a, i).start()

    def over_hidden(a, terms, keep):
        def one(i, core):
            owner = ((y + i) % ys_count) * CORES + core
            first = pl.multiple_of(owner * feat, feat)
            value = None
            for left, weight in terms:
                more = dot(left[pl.ds(0, rows_t), :], weight[pl.ds(first, feat), :], 1, 1)
                value = more if value is None else value + more
            return value

        order = list(range(1, ys_count)) + [0]
        for i in order:
            dg[pl.ds(a * rows_t, rows_t), pl.ds(i * feat, feat)] = one(i, 1 - c).astype(BF16)
            to_core(a, i).start()
        for i in order:
            if i == 0 or a == 0:
                keep[i if a == 0 else 0] = one(i, c)
            else:
                row_share(a, i, one(i, c))

    def received(a, own):
        to_core(a, 0).wait_recv()
        total = own[0] + mp_recv[a, 0].astype(F32)
        for i in range(1, ys_count):
            to_row(a, i).wait_recv()
            total = total + mp_recv[a, ys_count + i - 1].astype(F32)
        return total

    def shares_sent(a):
        for i in range(ys_count):
            to_core(a, i).wait_send()
        for i in range(1, ys_count):
            to_row(a, i).wait_send()

    pending = {}
    turn = [0]

    def own_rows(w):
        left, right = sides[w]
        for n in range(width // big):
            slot = turn[0] % 2
            if slot in pending:
                pending[slot].wait()
            lanes = pl.ds(n * big, big)
            stage[slot] = dot(left[pl.ds(0, rows), :], right[:, lanes])
            copy = pltpu.make_async_copy(stage.at[slot], own_hbm.at[w, :, lanes], o_sem.at[slot])
            copy.start()
            pending[slot] = copy
            turn[0] += 1

    transposed(hg, ht)
    for k in range(1, Z):
        forward_c(1, k, True)
    for k in range(1, Z):
        ready(1, k, True)
    transposed(dg, dt)
    own_sent(0)
    rest_sent(0)
    rs_compute(2, 0)
    rs_start(2, 0)
    hidden_half(3, steps // 2, steps)
    load_d = pltpu.make_async_copy(wd_hbm, wa, w_sem.at[0])
    load_d.start()
    at_once(inner & late, (pass_on, 2))
    at_once(outer & late, (take, 2), (take, 3))
    at_once(outer & alone, (take, 3))
    rs_compute(2, 1)
    rs_start(2, 1)
    load_d.wait()

    def gradient_part(k, first, last):
        part = pl.ds(k * rows_t, rows_t)

        def gradient_tile(n, carry):
            w = cols(n, tile)
            gh = dot(dg[part, :], wa[:, w])
            ggi[part, w] = (gh * ggi[part, w].astype(F32)).astype(BF16)
            gl[part, w] = (gh * gl[part, w].astype(F32)).astype(BF16)
            return carry

        lax.fori_loop(first, last, gradient_tile, 0)

    forward_c(1, 1, False)
    gradient_part(0, 0, steps)
    forward_c(1, 2, False)
    ready(1, 1, False)
    gradient_part(1, 0, steps)
    forward_c(1, 3, False)
    ready(1, 2, False)
    gradient_part(2, 0, steps)
    ready(1, 3, False)
    gradient_part(Z - 1, 0, steps // 2)
    rs_compute(0, 0)
    rs_start(0, 0)
    gradient_part(Z - 1, steps // 2, steps)
    rs_compute(1, 0)
    rs_start(1, 0)
    own_sent(1)
    rest_sent(1)
    over_hidden(0, ((hidden, wa),), own_b)
    load_g = pltpu.make_async_copy(wg_hbm, wa, w_sem.at[0])
    load_g.start()
    rs_compute(0, 1)
    rs_start(0, 1)
    rs_compute(1, 1)
    load_g.wait()
    over_hidden(1, ((ggi, wa), (gl, wb)), own_g)
    for i in range(1, ys_count):
        row_share(0, i, own_b[i])
    for w in range(3):
        own_rows(w)
    for copy in pending.values():
        copy.wait()
    own_g[0] = received(1, own_g)
    normed = x_ref[...].astype(F32) * per_token(sblk[...])
    part_x[x] = group_sums(own_g[0] * normed)
    exchange_start(part_x, x, px_s, px_r, xs, x_peer)
    rs_start(1, 1)
    part_z[z] = exchange_sum(part_x, x, px_s, px_r, xs, x_peer)
    exchange_start(part_z, z, pz_s, pz_r, Z, z_peer)
    total = exchange_sum(part_z, z, pz_s, pz_r, Z, z_peer)
    gg_ref[...] = jnp.sum(total, axis=0, keepdims=True)
    scale = per_token(sblk[...])
    normed = x_ref[...].astype(F32) * scale
    mean_term = per_token(per_block(gain * total / GHOST))
    gt_ref[...] = (
        dy_ref[...].astype(F32) + scale * (gain * own_g[0] - normed * mean_term)
    ).astype(BF16)
    bo_ref[...] = (x_ref[...].astype(F32) + received(0, own_b)).astype(BF16)
    shares_sent(0)
    shares_sent(1)
    for w in range(3):
        for j in range(1, xs):
            for h in range(halves):
                rs_copy(w, j, h).wait()


def finish(own, recv, bo, gt, rn, gg, bo_out, gt_out, rn_out, gg_out, dgate, dup, ddown):
    for w, out in enumerate((dgate, dup, ddown)):
        value = own[w]
        for j in range(recv.shape[1]):
            value = value + recv[w, j].astype(F32)
        out[...] = value

    @pl.when(pl.program_id(0) == 0)
    def _():
        bo_out[...] = bo[...]
        gt_out[...] = gt[...]
        rn_out[...] = rn[...]
        gg_out[...] = gg[...]


def body(tokens, norm_gain, running_sq, gate_weight, up_weight, down_weight_t, groups, cotangent):
    tok_count, mp_count = lax.axis_size("tok"), lax.axis_size("mp")
    rows_t, feat = tokens.shape
    full, width = gate_weight.shape
    xs = tok_count // Z
    rows = full // tok_count
    nb = rows_t // BLK
    groups_total = rows_t * tok_count // GHOST
    ys_count = mp_count // CORES
    big = min(512, width // 2)
    vmem = pl.BlockSpec(memory_space=pltpu.VMEM)
    hbm = pl.BlockSpec(memory_space=pl.ANY)
    dma = pltpu.SemaphoreType.DMA
    table = (groups_total, feat)
    small = (
        jax.ShapeDtypeStruct((rows_t, feat), BF16),
        jax.ShapeDtypeStruct((rows_t, feat), BF16),
        jax.ShapeDtypeStruct((1, feat), F32),
        jax.ShapeDtypeStruct((1, feat), F32),
    )
    outs = pl.pallas_call(
        functools.partial(kernel, tok_count, mp_count),
        out_shape=small
        + (
            jax.ShapeDtypeStruct((3, rows, width), F32),
            jax.ShapeDtypeStruct((3, xs - 1, rows, width), BF16),
        ),
        in_specs=[vmem] * 5 + [hbm] * 3,
        out_specs=(vmem,) * 4 + (hbm,) * 2,
        scratch_shapes=[
            pltpu.VMEM((full, width), BF16),
            pltpu.VMEM((full, width), BF16),
            pltpu.VMEM((Z * rows_t, full), BF16),
            pltpu.VMEM((Z * rows_t, full), BF16),
            pltpu.VMEM((Z * rows_t, width), BF16),
            pltpu.VMEM((Z * rows_t, width), BF16),
            pltpu.VMEM((Z * rows_t, width), BF16),
            pltpu.VMEM((xs * rows, Z * rows_t), BF16),
            pltpu.VMEM((xs * rows, Z * rows_t), BF16),
            pltpu.VMEM((2, mp_count - 1, rows_t, feat), BF16),
            pltpu.VMEM((2, rows, big), F32),
            pltpu.VMEM((nb, feat), F32),
            pltpu.VMEM((xs,) + table, F32),
            pltpu.VMEM((Z,) + table, F32),
            pltpu.VMEM((xs,) + table, F32),
            pltpu.VMEM((Z,) + table, F32),
            pltpu.VMEM((ys_count, rows_t, feat), F32),
            pltpu.VMEM((1, rows_t, feat), F32),
            dma((2,)),
            dma((2, 6)),
            dma((2, Z + 1)),
            dma((2, Z, ys_count)),
            dma((2, Z, ys_count)),
            dma((2, Z, ys_count)),
            dma((2, Z, ys_count)),
            dma((xs,)),
            dma((xs,)),
            dma((Z,)),
            dma((Z,)),
            dma((xs,)),
            dma((xs,)),
            dma((Z,)),
            dma((Z,)),
            dma((3, xs, 2)),
            dma((3, xs, 2)),
            dma((2, mp_count)),
            dma((2, mp_count)),
            dma((2,)),
        ],
        compiler_params=pltpu.CompilerParams(
            collective_id=0, has_side_effects=True, vmem_limit_bytes=67043328
        ),
        name="sublayer",
    )(
        tokens,
        norm_gain.reshape(mp_count, 1, feat),
        running_sq.reshape(1, feat),
        groups.reshape(1, nb),
        cotangent,
        gate_weight,
        up_weight,
        down_weight_t,
    )
    block_out, grad_tokens, running_new, grad_gain, own, recv = outs
    span = min(512, width)
    whole = [pl.BlockSpec(leaf.shape, lambda n: (0, 0)) for leaf in small]
    grad = jax.ShapeDtypeStruct((rows, width), F32)
    block_out, grad_tokens, running_new, grad_gain, grad_gate, grad_up, grad_down_t = pl.pallas_call(
        finish,
        grid=(width // span,),
        out_shape=small + (grad,) * 3,
        in_specs=[
            pl.BlockSpec((3, rows, span), lambda n: (0, 0, n)),
            pl.BlockSpec((3, xs - 1, rows, span), lambda n: (0, 0, 0, n)),
        ]
        + whole,
        out_specs=whole + [pl.BlockSpec((rows, span), lambda n: (0, n))] * 3,
        name="finish",
    )(own, recv, block_out, grad_tokens, running_new, grad_gain)
    return (
        block_out,
        grad_tokens,
        running_new.reshape(feat),
        grad_gain.reshape(feat),
        grad_gate,
        grad_up,
        grad_down_t,
    )


def solution(mesh):
    placed = (
        P("tok", "mp"),
        P(),
        P("mp"),
        P(None, "mp"),
        P(None, "mp"),
        P(None, "mp"),
        P("tok"),
        P("tok", "mp"),
    )
    return jax.shard_map(
        body,
        mesh=mesh,
        in_specs=placed,
        out_specs=(
            P("tok", "mp"),
            P("tok", "mp"),
            P("mp"),
            P("mp"),
            P("tok", "mp"),
            P("tok", "mp"),
            P("tok", "mp"),
        ),
        check_vma=False,
    )
```
